256 devices in a mesh: row: 8 (over x, core), col: 32 (over y, z).
Axes of the slice: x: 4, y: 4, z: 8, core: 2. Of those that a mesh axis runs over, the one named last changes fastest.
Arguments:
- tensor: float32 [1024, 64, 4096], P(None, 'row', 'col'), may hold values from -60 to 60, as said below
- factor_two: float32 [64, 32], P('row'), may hold values from -0.75 to 0.75
- factor_three: float32 [128, 32], P('col'), may hold values from -0.5 to 0.5
- factor_four: float32 [32, 16], replicated, may hold values from -1 to 1
- factor_init: float32 [1024, 64], replicated, may hold values from -6 to 6
Outputs:
- factor_new: float32 [1024, 64], replicated
- core: float32 [64, 32, 32, 16], P(None, 'row', 'col')
The draws below stay inside these ranges and needn't reach their ends.
Inputs may be any that keep to these rules, and one draw needn't show every extreme that they name: `tensor`: scales vary from slab to slab.
All inputs are finite; a program needn't handle non-finite values.
Results may differ from the reference program's by a relative error of at most 0.00013.
Values sent between devices are 32-bit elements; how exact they have to be, the bound alone decides.
No kernel may reach another device: no remote copies, remote signals or barrier semaphores. Data moves between devices by JAX's collectives and lax.ppermute only.
A program may use at most 128 MiB of HBM per device.

```python
import jax
import jax.numpy as jnp
from jax import lax

I1 = 1024
I4 = 32
R1 = 64
R2 = 32
R3 = 32
R4 = 16
ITERS = 1
I2 = 64
I3 = 128


def draw_tensor(key, part):
    first, second = jax.random.split(jax.random.fold_in(key, 11), 2)
    shape = (I1, I2, I3 * I4)
    base = jnp.clip(jax.random.normal(first, shape, jnp.float32), -6.0, 6.0)
    ramp_two = jnp.arange(I2, dtype=jnp.float32) / max(I2 - 1, 1)
    ramp_three = jnp.arange(I3, dtype=jnp.float32) / max(I3 - 1, 1)
    logs = jax.random.uniform(second, (I2, I3), jnp.float32) + 0.5 * ramp_two[:, None] + 0.5 * ramp_three[None, :] - 1.0
    scales = jnp.repeat(10.0 ** logs, I4, axis=1)
    values = base * scales[None, :, :]
    return jnp.clip(values, -60.0, 60.0)


def levels(key, dims, cuts, smallest, high):
    loudness = 1.0
    for dim, blocks in cuts:
        draws = jax.random.uniform(jax.random.fold_in(jax.random.fold_in(key, 6), dim), (blocks,), jnp.float32, smallest / len(cuts), high / len(cuts))
        loudness = loudness * jnp.repeat(jnp.exp(draws), dims[dim] // blocks).reshape((-1,) + (1,) * (len(dims) - 1 - dim))
    return loudness


def bell_draw(rng, extent, spread, limit, shards=(), kind=jnp.bfloat16):
    level = levels(rng, extent, shards, -0.22, 0.18) if shards else 1.0
    array = jax.random.normal(rng, extent, jnp.float32) * spread * level
    return jnp.minimum(jnp.maximum(array, -limit), limit).astype(kind)


def setup_inputs(seed: int = 0) -> dict:
    key_list = jax.random.split(jax.random.key(seed), 6)
    tensor = draw_tensor(jax.random.fold_in(key_list[5], 71), 0)
    factor_two = bell_draw(key_list[1], (I2, R2), I2 ** -0.5, 0.75, ((0, 8),), jnp.float32)
    factor_three = bell_draw(key_list[2], (I3, R3), I3 ** -0.5, 0.5, ((0, 32),), jnp.float32)
    factor_four = bell_draw(key_list[3], (I4, R4), I4 ** -0.5, 1.0, (), jnp.float32)
    factor_init = bell_draw(key_list[4], (I1, R1), 1.0, 6.0, (), jnp.float32)
    return dict(tensor=tensor, factor_two=factor_two, factor_three=factor_three, factor_four=factor_four, factor_init=factor_init)


def reference(tensor, factor_two, factor_three, factor_four, factor_init):
    highest = lax.Precision.HIGHEST
    data = tensor.reshape(I1, I2, I3, I4)
    fourth = jnp.einsum('abcd,de->abce', data, factor_four, precision=highest)
    third = jnp.einsum('abce,cf->abfe', fourth, factor_three, precision=highest)
    projected = jnp.einsum('abfe,bg->agfe', third, factor_two, precision=highest)
    unfolded = projected.reshape(I1, R2 * R3 * R4)
    gram = jnp.dot(unfolded.astype(jnp.float32), unfolded.T.astype(jnp.float32), precision=highest, preferred_element_type=jnp.float32)
    basis = factor_init
    for step in range(ITERS):
        image = jnp.dot(gram.astype(jnp.float32), basis.astype(jnp.float32), precision=highest, preferred_element_type=jnp.float32)
        square = jnp.dot(image.T.astype(jnp.float32), image.astype(jnp.float32), precision=highest, preferred_element_type=jnp.float32)
        lower = jnp.linalg.cholesky(square)
        basis = jax.scipy.linalg.solve_triangular(lower, image.T, lower=True).T
    core = jnp.dot(basis.T.astype(jnp.float32), unfolded.astype(jnp.float32), precision=highest, preferred_element_type=jnp.float32)
    return (basis, core.reshape(R1, R2, R3, R4))
```

```python
import functools

import jax
import jax.numpy as jnp
from jax import lax
from jax.experimental import pallas as pl
from jax.experimental.pallas import tpu as pltpu
from jax.sharding import Mesh
from jax.sharding import PartitionSpec as P

ROW = ("x", "k")
COL = ("y", "z")
PLANE = ("x", "k", "y")
F32 = jnp.float32


def mm(a, b, left=1, right=0):
    return lax.dot_general(
        a, b, (((left,), (right,)), ((), ())),
        precision=lax.Precision.HIGHEST, preferred_element_type=F32,
    )


def call(body, outs, smem=(), n_in=0, flops=0):
    vm = pl.BlockSpec(memory_space=pltpu.VMEM)
    sm = pl.BlockSpec(memory_space=pltpu.SMEM)
    return pl.pallas_call(
        body,
        out_shape=[jax.ShapeDtypeStruct(s, F32) for s in outs],
        in_specs=[sm if i in smem else vm for i in range(n_in)],
        out_specs=[vm] * len(outs),
        cost_estimate=pl.CostEstimate(flops=flops, bytes_accessed=1 << 20, transcendentals=0),
    )


def first_mode(bt, x_ref, k4t):
    combs = []
    for b in range(0, 8, 2):
        pair = jnp.concatenate(
            [x_ref[pl.ds(b, 1024, stride=8), :], x_ref[pl.ds(b + 1, 1024, stride=8), :]], axis=1
        )
        z = mm(bt, pair)
        for h in range(2):
            m = mm(k4t, z[:, h * 128 : (h + 1) * 128], 1, 1)
            combs.append(jnp.concatenate([m[:32], m[32:]], axis=1))
    return combs


def start_body(x_ref, bt_ref, k4t_ref, f2_ref, out_ref):
    combs = first_mode(bt_ref[...], x_ref, k4t_ref[...])
    for b, comb in enumerate(combs):
        for c in range(4):
            out_ref[pl.ds(c * 8 + b, 8, stride=40), :] = comb[c * 8 : (c + 1) * 8]
    tail = jnp.concatenate([f2_ref[...], jnp.zeros((8, 96), F32)], axis=1)
    for i in range(8):
        out_ref[i * 40 + 32 : i * 40 + 40, :] = tail


def second_body(r_ref, f3_ref, out_ref, f2_ref):
    f2 = r_ref[:, 32:40, :].reshape(64, 128)[:, :32]
    f2_ref[...] = f2
    data = jnp.concatenate([r_ref[:, c * 8 : (c + 1) * 8, :].reshape(64, 128) for c in range(4)], axis=1)
    y = mm(f2, data, 0, 0)
    f3 = jnp.concatenate([f3_ref[...], jnp.zeros((4, 96), F32)], axis=1)
    for c in range(4):
        out_ref[pl.ds(c, 32, stride=8), :] = y[:, c * 128 : (c + 1) * 128]
        out_ref[pl.ds(4 + c, 32, stride=8), :] = jnp.broadcast_to(f3[c : c + 1], (32, 128))


def third_body(r_ref, out_ref):
    data = jnp.concatenate([r_ref[pl.ds(c, 32, stride=8), :] for c in range(4)], axis=0)
    f3 = jnp.concatenate([r_ref[pl.ds(4 + c, 32, stride=8), :] for c in range(4)], axis=0)[:, :32]
    q = mm(f3, mm(f3, data, 0, 0))
    for c in range(4):
        out_ref[pl.ds(c, 32, stride=4), :] = q[c * 32 : (c + 1) * 32]


def back_body(r_ref, f2_ref, out_ref):
    data = jnp.concatenate([r_ref[pl.ds(c, 32, stride=4), :] for c in range(4)], axis=1)
    y = mm(f2_ref[...], data)
    for c in range(4):
        out_ref[:, c * 8 : (c + 1) * 8, :] = y[:, c * 128 : (c + 1) * 128].reshape(8, 8, 128)


def image_body(r_ref, k4t_ref, x_ref, out_ref):
    top = jnp.zeros((512, 64), F32)
    low = jnp.zeros((512, 64), F32)
    for b in range(0, 8, 2):
        ws = []
        for h in range(2):
            w4 = jnp.concatenate([r_ref[pl.ds(c * 8 + b + h, 8, stride=32), :] for c in range(4)], axis=0)
            w4 = jnp.concatenate([w4[:, :64], w4[:, 64:]], axis=0)
            ws.append(mm(k4t_ref[...], w4, 0, 0))
        w = jnp.concatenate(ws, axis=0)
        pair = jnp.concatenate(
            [x_ref[pl.ds(b, 1024, stride=8), :], x_ref[pl.ds(b + 1, 1024, stride=8), :]], axis=1
        )
        full = mm(pair, w)
        top, low = top + full[:512], low + full[512:]
    out_ref[...] = jnp.concatenate([top, low], axis=1)


def sum_body(r_ref, out_ref):
    total = r_ref[0]
    for i in range(1, r_ref.shape[0]):
        total = total + r_ref[i]
    for i in range(out_ref.shape[0]):
        out_ref[i] = total


def core_two_body(image_ref, x_ref, k4t_ref, f2_ref, out_ref, turned_ref):
    flat = image_ref[...].T
    bt = jnp.concatenate([flat[:64], flat[64:]], axis=1)
    turned_ref[...] = bt
    combs = first_mode(bt, x_ref, k4t_ref[...])
    for g in range(32):
        total = f2_ref[0, g] * combs[0]
        for b in range(1, 8):
            total = total + f2_ref[b, g] * combs[b]
        out_ref[g * 32 : (g + 1) * 32, :] = total


def core_three_body(r_ref, f3_ref, out_ref):
    total = r_ref[0]
    for i in range(1, 8):
        total = total + r_ref[i]
    for f in range(32):
        for g in range(4):
            piece = f3_ref[0, f] * total[g * 32 : g * 32 + 8]
            for c in range(1, 4):
                piece = piece + f3_ref[c, f] * total[g * 32 + c * 8 : g * 32 + c * 8 + 8]
            out_ref[(f * 4 + g) * 8 : (f * 4 + g + 1) * 8, :] = piece


def core_body(r_ref, linv_ref, out_ref):
    total = r_ref[0]
    for i in range(1, 32):
        total = total + r_ref[i]
    parts = []
    for g in range(4):
        parts += [total[g * 8 : g * 8 + 8, :64], total[g * 8 : g * 8 + 8, 64:]]
    out_ref[...] = mm(jnp.concatenate(parts, axis=0), linv_ref[...], 1, 1)


def trade(block, axis):
    return lax.all_to_all(block, axis, split_axis=0, concat_axis=0, tiled=True)


def shards(tensor, factor_two, factor_three, factor_four, factor_init):
    x = tensor.reshape(8192, 128)
    k4t = (
        factor_four.T.reshape(2, 1, 8, 1, 32) * jnp.eye(4, dtype=F32).reshape(1, 4, 1, 4, 1)
    ).reshape(64, 128)
    (block,) = call(start_body, [(320, 128)], n_in=4, flops=10**9)(x, factor_init.T, k4t, factor_two)
    block = trade(block.reshape(8, 40, 128), ROW)
    block, whole_two = call(second_body, [(256, 128), (64, 32)], n_in=2, flops=10**7)(block, factor_three)
    block = trade(block.reshape(32, 8, 128), COL)
    (block,) = call(third_body, [(128, 128)], n_in=1, flops=10**7)(block.reshape(256, 128))
    block = trade(block.reshape(32, 4, 128), COL)
    (block,) = call(back_body, [(8, 32, 128)], n_in=2, flops=10**7)(block.reshape(128, 128), whole_two)
    block = trade(block, ROW)
    (image,) = call(image_body, [(512, 128)], n_in=3, flops=10**9)(block.reshape(256, 128), k4t, x)
    image = trade(image.reshape(32, 16, 128), PLANE)
    (image,) = call(sum_body, [(8, 16, 128)], n_in=1, flops=10**6)(image)
    image = trade(image, "z")
    (image,) = call(sum_body, [(32, 16, 128)], n_in=1, flops=10**6)(image)
    image = trade(image, PLANE)
    block, turned = call(core_two_body, [(1024, 128), (64, 1024)], smem=(3,), n_in=4, flops=10**9)(
        image.reshape(512, 128), x, k4t, factor_two
    )
    block = trade(block.reshape(8, 128, 128), ROW)
    square = mm(turned, turned, 1, 1)
    lower = jnp.linalg.cholesky(square)
    linv = jax.scipy.linalg.solve_triangular(lower, jnp.eye(64, dtype=F32), lower=True)
    basis = mm(linv, turned)
    (block,) = call(core_three_body, [(1024, 128)], smem=(1,), n_in=2, flops=10**7)(block, factor_three)
    block = trade(block.reshape(32, 32, 128), COL)
    (core,) = call(core_body, [(64, 64)], n_in=2, flops=10**7)(block, linv)
    return basis.T, core.reshape(4, 1, 16, 64).transpose(3, 0, 1, 2)


def solution(mesh):
    split = Mesh(mesh.devices.reshape(4, 2, 4, 8), ("x", "k", "y", "z"))
    in_specs = (P(None, ROW, COL), P(ROW, None), P(COL, None), P(), P())
    out_specs = (P(), P(None, ROW, COL, None))
    return jax.shard_map(shards, mesh=split, in_specs=in_specs, out_specs=out_specs, check_vma=False)
```

```python
import jax
import jax.numpy as jnp
from jax import lax
from jax.experimental import pallas as pl
from jax.experimental.pallas import tpu as pltpu
from jax.sharding import Mesh
from jax.sharding import PartitionSpec as P

ROW = ("x", "k")
COL = ("y", "z")
PLANE = ("x", "k", "y")
F32 = jnp.float32
BF16 = jnp.bfloat16
HBM = pltpu.HBM
VMEM = pltpu.VMEM
SMEM = pltpu.SMEM


def mm(a, b, left=1, right=0):
    return lax.dot_general(
        a, b, (((left,), (right,)), ((), ())),
        precision=lax.Precision.HIGHEST, preferred_element_type=F32,
    )


def mm16(a, b):
    return jnp.dot(a, b, preferred_element_type=F32)


def halves(a):
    high = a.astype(BF16)
    return high, (a - high.astype(F32)).astype(BF16)


def call(body, outs, spaces, scratch=(), mib=4, flops=0):
    vmem = pl.BlockSpec(memory_space=pltpu.VMEM)
    specs = [pl.BlockSpec(memory_space=s) for s in spaces]
    return pl.pallas_call(
        body,
        out_shape=[jax.ShapeDtypeStruct(s, d) for s, d in outs],
        in_specs=specs,
        out_specs=[vmem] * len(outs),
        scratch_shapes=list(scratch),
        compiler_params=pltpu.CompilerParams(vmem_limit_bytes=mib << 20),
        cost_estimate=pl.CostEstimate(flops=flops, bytes_accessed=1 << 20, transcendentals=0),
    )


def fourth_matrix(f4t):
    wide = jnp.concatenate([f4t] * 4, axis=1)
    owner = lax.broadcasted_iota(jnp.int32, (8, 128), 1) // 32
    rows = [
        jnp.where(owner == c, wide[lo * 8 : lo * 8 + 8], 0.0) for lo in range(2) for c in range(4)
    ]
    return jnp.concatenate(rows, axis=0)


def fourth_mode(z, k4t):
    stack = jnp.concatenate([z[:, b * 128 : (b + 1) * 128] for b in range(8)], axis=0)
    m = mm(k4t, stack, 1, 1)
    return [
        jnp.concatenate([m[:32, b * 64 : b * 64 + 64], m[32:, b * 64 : b * 64 + 64]], axis=1)
        for b in range(8)
    ]


def start_body(x_ref, bt_ref, f4t_ref, f2_ref, out_ref, high_ref, low_ref, k4t_ref, held, sems):
    def copy(i):
        part = pl.ds(i * 2048, 2048)
        return pltpu.make_async_copy(x_ref.at[part], held.at[part], sems.at[i])

    for i in range(4):
        copy(i).start()
    k4t = fourth_matrix(f4t_ref[...])
    k4t_ref[...] = k4t
    tail = jnp.concatenate([f2_ref[...], jnp.zeros((8, 96), F32)], axis=1)
    for i in range(8):
        out_ref[i * 40 + 32 : i * 40 + 40, :] = tail
    bt_high, bt_low = halves(bt_ref[...])
    both = jnp.concatenate([bt_high, bt_low], axis=0)
    z = jnp.zeros((64, 1024), F32)
    for i in range(4):
        copy(i).wait()
        rows = slice(i * 256, i * 256 + 256)
        for b in range(8):
            high, low = halves(held[pl.ds(i * 2048 + b, 256, stride=8), :])
            high_ref[rows, b * 128 : b * 128 + 128] = high
            low_ref[rows, b * 128 : b * 128 + 128] = low
        major = mm16(both[:, rows], high_ref[rows, :])
        z = z + major[:64] + major[64:] + mm16(bt_high[:, rows], low_ref[rows, :])
    for b, comb in enumerate(fourth_mode(z, k4t)):
        for c in range(4):
            out_ref[pl.ds(c * 8 + b, 8, stride=40), :] = comb[c * 8 : (c + 1) * 8]


def second_body(r_ref, f3_ref, out_ref, f2_ref):
    f2 = r_ref[:, 32:40, :].reshape(64, 128)[:, :32]
    f2_ref[...] = f2
    data = jnp.concatenate([r_ref[:, c * 8 : (c + 1) * 8, :].reshape(64, 128) for c in range(4)], axis=1)
    y = mm(f2, data, 0, 0)
    f3 = jnp.concatenate([f3_ref[...], jnp.zeros((4, 96), F32)], axis=1)
    for c in range(4):
        out_ref[pl.ds(c, 32, stride=8), :] = y[:, c * 128 : (c + 1) * 128]
        out_ref[pl.ds(4 + c, 32, stride=8), :] = jnp.broadcast_to(f3[c : c + 1], (32, 128))


def third_body(r_ref, out_ref):
    data = jnp.concatenate([r_ref[pl.ds(c, 32, stride=8), :] for c in range(4)], axis=0)
    f3 = jnp.concatenate([r_ref[pl.ds(4 + c, 32, stride=8), :] for c in range(4)], axis=0)[:, :32]
    q = mm(f3, mm(f3, data, 0, 0))
    for c in range(4):
        out_ref[pl.ds(c, 32, stride=4), :] = q[c * 32 : (c + 1) * 32]


def back_body(r_ref, f2_ref, out_ref):
    data = jnp.concatenate([r_ref[pl.ds(c, 32, stride=4), :] for c in range(4)], axis=1)
    y = mm(f2_ref[...], data)
    for c in range(4):
        out_ref[:, c * 8 : (c + 1) * 8, :] = y[:, c * 128 : (c + 1) * 128].reshape(8, 8, 128)


def image_body(r_ref, k4t_ref, high_ref, low_ref, out_ref):
    ws = []
    for b in range(8):
        w4 = jnp.concatenate([r_ref[pl.ds(c * 8 + b, 8, stride=32), :] for c in range(4)], axis=0)
        ws.append(jnp.concatenate([w4[:, :64], w4[:, 64:]], axis=0))
    w = mm(k4t_ref[...], jnp.concatenate(ws, axis=1), 0, 0)
    w = jnp.concatenate([w[:, b * 64 : b * 64 + 64] for b in range(8)], axis=0)
    w_high, w_low = halves(w)
    none = jnp.zeros((1024, 64), BF16)
    first = jnp.concatenate([w_high, w_low], axis=1)
    second = jnp.concatenate([w_low, w_high], axis=1)
    left = jnp.concatenate([w_high, none], axis=1)
    right = jnp.concatenate([none, w_high], axis=1)
    half = lax.broadcasted_iota(jnp.int32, (128, 128), 1) < 64
    for i in range(4):
        top = slice(i * 128, i * 128 + 128)
        low = slice(512 + i * 128, 512 + i * 128 + 128)
        t = mm16(high_ref[top, :], first)
        u = mm16(high_ref[low, :], second)
        rest = mm16(low_ref[top, :], left) + mm16(low_ref[low, :], right)
        out_ref[top, :] = jnp.where(half, t, u) + pltpu.roll(jnp.where(half, u, t), 64, 1) + rest


def sum_body(r_ref, out_ref):
    total = r_ref[0]
    for i in range(1, r_ref.shape[0]):
        total = total + r_ref[i]
    for i in range(out_ref.shape[0]):
        out_ref[i] = total


def core_two_body(image_ref, high_ref, low_ref, k4t_ref, f2_ref, out_ref, turned_ref):
    flat = image_ref[...].T
    bt = jnp.concatenate([flat[:64], flat[64:]], axis=1)
    turned_ref[...] = bt
    bt_high, bt_low = halves(bt)
    major = mm16(jnp.concatenate([bt_high, bt_low], axis=0), high_ref[...])
    z = major[:64] + major[64:] + mm16(bt_high, low_ref[...])
    combs = fourth_mode(z, k4t_ref[...])
    for g in range(32):
        total = f2_ref[0, g] * combs[0]
        for b in range(1, 8):
            total = total + f2_ref[b, g] * combs[b]
        out_ref[g * 32 : (g + 1) * 32, :] = total


def core_three_body(r_ref, f3_ref, out_ref):
    total = r_ref[0]
    for i in range(1, 8):
        total = total + r_ref[i]
    for f in range(32):
        for g in range(4):
            piece = f3_ref[0, f] * total[g * 32 : g * 32 + 8]
            for c in range(1, 4):
                piece = piece + f3_ref[c, f] * total[g * 32 + c * 8 : g * 32 + c * 8 + 8]
            out_ref[(f * 4 + g) * 8 : (f * 4 + g + 1) * 8, :] = piece


def core_body(r_ref, linv_ref, out_ref):
    total = r_ref[0]
    for i in range(1, 32):
        total = total + r_ref[i]
    parts = []
    for g in range(4):
        parts += [total[g * 8 : g * 8 + 8, :64], total[g * 8 : g * 8 + 8, 64:]]
    out_ref[...] = mm(jnp.concatenate(parts, axis=0), linv_ref[...], 1, 1)


def trade(block, axis):
    return lax.all_to_all(block, axis, split_axis=0, concat_axis=0, tiled=True)


def shards(tensor, factor_two, factor_three, factor_four, factor_init):
    x = tensor.reshape(8192, 128)
    block, high, low, k4t = call(
        start_body,
        [((320, 128), F32), ((1024, 1024), BF16), ((1024, 1024), BF16), ((64, 128), F32)],
        (HBM, VMEM, VMEM, VMEM),
        scratch=(pltpu.VMEM((8192, 128), F32), pltpu.SemaphoreType.DMA((4,))),
        mib=48, flops=10**9,
    )(x, factor_init.T, factor_four.T, factor_two)
    block = trade(block.reshape(8, 40, 128), ROW)
    block, whole_two = call(second_body, [((256, 128), F32), ((64, 32), F32)], (VMEM, VMEM), flops=10**7)(
        block, factor_three
    )
    block = trade(block.reshape(32, 8, 128), COL)
    (block,) = call(third_body, [((128, 128), F32)], (VMEM,), flops=10**7)(block.reshape(256, 128))
    block = trade(block.reshape(32, 4, 128), COL)
    (block,) = call(back_body, [((8, 32, 128), F32)], (VMEM, VMEM), flops=10**7)(block.reshape(128, 128), whole_two)
    block = trade(block, ROW)
    (image,) = call(image_body, [((512, 128), F32)], (VMEM,) * 4, mib=12, flops=10**9)(
        block.reshape(256, 128), k4t, high, low
    )
    image = trade(image.reshape(32, 16, 128), PLANE)
    (image,) = call(sum_body, [((8, 16, 128), F32)], (VMEM,), flops=10**6)(image)
    image = trade(image, "z")
    (image,) = call(sum_body, [((32, 16, 128), F32)], (VMEM,), flops=10**6)(image)
    image = trade(image, PLANE)
    block, turned = call(
        core_two_body, [((1024, 128), F32), ((64, 1024), F32)], (VMEM,) * 4 + (SMEM,), mib=12, flops=10**9
    )(image.reshape(512, 128), high, low, k4t, factor_two)
    block = trade(block.reshape(8, 128, 128), ROW)
    square = mm(turned, turned, 1, 1)
    lower = jnp.linalg.cholesky(square)
    linv = jax.scipy.linalg.solve_triangular(lower, jnp.eye(64, dtype=F32), lower=True)
    basis = mm(linv, turned)
    (block,) = call(core_three_body, [((1024, 128), F32)], (VMEM, SMEM), flops=10**7)(block, factor_three)
    block = trade(block.reshape(32, 32, 128), COL)
    (core,) = call(core_body, [((64, 64), F32)], (VMEM, VMEM), flops=10**7)(block, linv)
    return basis.T, core.reshape(4, 1, 16, 64).transpose(3, 0, 1, 2)


def solution(mesh):
    split = Mesh(mesh.devices.reshape(4, 2, 4, 8), ("x", "k", "y", "z"))
    in_specs = (P(None, ROW, COL), P(ROW, None), P(COL, None), P(), P())
    out_specs = (P(), P(None, ROW, COL, None))
    return jax.shard_map(shards, mesh=split, in_specs=in_specs, out_specs=out_specs, check_vma=False)
```

```python
import jax
import jax.numpy as jnp
from jax import lax
from jax.experimental import pallas as pl
from jax.experimental.pallas import tpu as pltpu
from jax.sharding import Mesh
from jax.sharding import PartitionSpec as P

ROW = ("x", "k")
COL = ("y", "z")
PLANE = ("x", "k", "y")
F32 = jnp.float32
BF16 = jnp.bfloat16
HBM = pltpu.HBM
VMEM = pltpu.VMEM
SMEM = pltpu.SMEM


def mm(a, b, left=1, right=0):
    return lax.dot_general(
        a, b, (((left,), (right,)), ((), ())),
        precision=lax.Precision.HIGHEST, preferred_element_type=F32,
    )


def mm16(a, b):
    return jnp.dot(a, b, preferred_element_type=F32)


def halves(a):
    high = a.astype(BF16)
    return high, (a - high.astype(F32)).astype(BF16)


def call(body, outs, spaces, scratch=(), mib=4, flops=0):
    vmem = pl.BlockSpec(memory_space=pltpu.VMEM)
    specs = [pl.BlockSpec(memory_space=s) for s in spaces]
    return pl.pallas_call(
        body,
        out_shape=[jax.ShapeDtypeStruct(s, d) for s, d in outs],
        in_specs=specs,
        out_specs=[vmem] * len(outs),
        scratch_shapes=list(scratch),
        compiler_params=pltpu.CompilerParams(vmem_limit_bytes=mib << 20),
        cost_estimate=pl.CostEstimate(flops=flops, bytes_accessed=1 << 20, transcendentals=0),
    )


def fourth_matrix(f4t):
    wide = jnp.concatenate([f4t] * 4, axis=1)
    owner = lax.broadcasted_iota(jnp.int32, (8, 128), 1) // 32
    rows = [
        jnp.where(owner == c, wide[lo * 8 : lo * 8 + 8], 0.0) for lo in range(2) for c in range(4)
    ]
    return jnp.concatenate(rows, axis=0)


def fourth_mode(z, k4t):
    stack = jnp.concatenate([z[:, b * 128 : (b + 1) * 128] for b in range(8)], axis=0)
    m = mm(k4t, stack, 1, 1)
    return [
        jnp.concatenate([m[:32, b * 64 : b * 64 + 64], m[32:, b * 64 : b * 64 + 64]], axis=1)
        for b in range(8)
    ]


def split_body(x_ref, high_ref, low_ref, held, sems):
    def copy(i):
        part = pl.ds(i * 1024, 1024)
        return pltpu.make_async_copy(x_ref.at[part], held.at[part], sems.at[i])

    for i in range(8):
        copy(i).start()
    for i in range(8):
        copy(i).wait()
        rows = slice(i * 128, i * 128 + 128)
        for b in range(8):
            high, low = halves(held[pl.ds(i * 1024 + b, 128, stride=8), :])
            high_ref[rows, b * 128 : b * 128 + 128] = high
            low_ref[rows, b * 128 : b * 128 + 128] = low


def first_mode(bt, high_ref, low_ref):
    bt_high, bt_low = halves(bt)
    major = mm16(jnp.concatenate([bt_high, bt_low], axis=0), high_ref[...])
    return major[:64] + major[64:] + mm16(bt_high, low_ref[...])


def start_body(high_ref, low_ref, bt_ref, f4t_ref, f2_ref, out_ref, k4t_ref):
    k4t = fourth_matrix(f4t_ref[...])
    k4t_ref[...] = k4t
    tail = jnp.concatenate([f2_ref[...], jnp.zeros((8, 96), F32)], axis=1)
    for i in range(8):
        out_ref[i * 40 + 32 : i * 40 + 40, :] = tail
    z = first_mode(bt_ref[...], high_ref, low_ref)
    for b, comb in enumerate(fourth_mode(z, k4t)):
        for c in range(4):
            out_ref[pl.ds(c * 8 + b, 8, stride=40), :] = comb[c * 8 : (c + 1) * 8]


def second_body(r_ref, f3_ref, out_ref, f2_ref, twice_ref):
    f2 = r_ref[:, 32:40, :].reshape(64, 128)[:, :32]
    f2_ref[...] = f2
    data = jnp.concatenate([r_ref[:, c * 8 : (c + 1) * 8, :].reshape(64, 128) for c in range(4)], axis=1)
    y = mm(f2, data, 0, 0)
    f3 = jnp.concatenate([f3_ref[...], jnp.zeros((4, 96), F32)], axis=1)
    for c in range(4):
        out_ref[pl.ds(c, 32, stride=8), :] = y[:, c * 128 : (c + 1) * 128]
        out_ref[pl.ds(4 + c, 32, stride=8), :] = jnp.broadcast_to(f3[c : c + 1], (32, 128))
    g = lax.broadcasted_iota(jnp.int32, (32, 64), 0)
    slot = lax.broadcasted_iota(jnp.int32, (32, 64), 1)
    twice_ref[...] = mm(f2, jnp.where(slot // 8 * 4 + slot % 4 == g, 1.0, 0.0).astype(F32))


def third_body(r_ref, out_ref):
    data = jnp.concatenate([r_ref[pl.ds(c, 32, stride=8), :] for c in range(4)], axis=0)
    f3 = jnp.concatenate([r_ref[pl.ds(4 + c, 32, stride=8), :] for c in range(4)], axis=0)[:, :32]
    q = mm(f3, mm(f3, data, 0, 0))
    for c in range(4):
        out_ref[pl.ds(c, 32, stride=4), :] = q[c * 32 : (c + 1) * 32]


def back_body(r_ref, f2_ref, out_ref):
    data = jnp.concatenate([r_ref[pl.ds(c, 32, stride=4), :] for c in range(4)], axis=1)
    y = mm(f2_ref[...], data)
    for c in range(4):
        out_ref[:, c * 8 : (c + 1) * 8, :] = y[:, c * 128 : (c + 1) * 128].reshape(8, 8, 128)


def image_body(r_ref, k4t_ref, high_ref, low_ref, out_ref):
    ws = []
    for b in range(8):
        w4 = jnp.concatenate([r_ref[pl.ds(c * 8 + b, 8, stride=32), :] for c in range(4)], axis=0)
        ws.append(jnp.concatenate([w4[:, :64], w4[:, 64:]], axis=0))
    w = mm(k4t_ref[...], jnp.concatenate(ws, axis=1), 0, 0)
    w = jnp.concatenate([w[:, b * 64 : b * 64 + 64] for b in range(8)], axis=0)
    w_high, w_low = halves(w)
    none = jnp.zeros((1024, 64), BF16)
    first = jnp.concatenate([w_high, w_low], axis=1)
    second = jnp.concatenate([w_low, w_high], axis=1)
    left = jnp.concatenate([w_high, none], axis=1)
    right = jnp.concatenate([none, w_high], axis=1)
    half = lax.broadcasted_iota(jnp.int32, (128, 128), 1) < 64
    for i in range(4):
        top = slice(i * 128, i * 128 + 128)
        low = slice(512 + i * 128, 512 + i * 128 + 128)
        t = mm16(high_ref[top, :], first)
        u = mm16(high_ref[low, :], second)
        rest = mm16(low_ref[top, :], left) + mm16(low_ref[low, :], right)
        out_ref[top, :] = jnp.where(half, t, u) + pltpu.roll(jnp.where(half, u, t), 64, 1) + rest


def sum_body(r_ref, out_ref):
    total = r_ref[0]
    for i in range(1, r_ref.shape[0]):
        total = total + r_ref[i]
    for i in range(out_ref.shape[0]):
        out_ref[i] = total


def core_two_body(image_ref, high_ref, low_ref, k4t_ref, out_ref, turned_ref):
    flat = image_ref[...].T
    bt = jnp.concatenate([flat[:64], flat[64:]], axis=1)
    turned_ref[...] = bt
    z = first_mode(bt, high_ref, low_ref)
    for b, comb in enumerate(fourth_mode(z, k4t_ref[...])):
        for c in range(4):
            out_ref[pl.ds(c * 8 + b, 8, stride=32), :] = comb[c * 8 : (c + 1) * 8]


def core_three_body(r_ref, twice_ref, f3_ref, out_ref):
    data = jnp.concatenate([r_ref[:, c * 8 : (c + 1) * 8, :].reshape(64, 128) for c in range(4)], axis=1)
    y = mm(twice_ref[...], data, 0, 0)
    upper = lax.broadcasted_iota(jnp.int32, (8, 128), 0) < 4
    for f in range(0, 32, 2):
        scale = [jnp.where(upper, f3_ref[c, f], f3_ref[c, f + 1]) for c in range(4)]
        for i in range(8):
            piece = scale[0] * y[i * 8 : i * 8 + 8, :128]
            for c in range(1, 4):
                piece = piece + scale[c] * y[i * 8 : i * 8 + 8, c * 128 : c * 128 + 128]
            out_ref[(i * 32 + f) * 4 : (i * 32 + f) * 4 + 8, :] = piece


def core_body(r_ref, linv_ref, out_ref, kept):
    for i in range(8):
        total = r_ref[i * 128 : i * 128 + 8, :]
        for t in range(1, 16):
            total = total + r_ref[i * 128 + t * 8 : i * 128 + t * 8 + 8, :]
        kept[i * 8 : i * 8 + 8, :] = total + pltpu.roll(total, 4, 0)
    parts = []
    for g in range(4):
        tile = kept[pl.ds(g, 8, stride=8), :]
        parts += [tile[:, :64], tile[:, 64:]]
    out_ref[...] = mm(jnp.concatenate(parts, axis=0), linv_ref[...], 1, 1)


def trade(block, axis):
    return lax.all_to_all(block, axis, split_axis=0, concat_axis=0, tiled=True)


def shards(tensor, factor_two, factor_three, factor_four, factor_init):
    x = tensor.reshape(8192, 128)
    high, low = call(
        split_body, [((1024, 1024), BF16)] * 2, (HBM,),
        scratch=(pltpu.VMEM((8192, 128), F32), pltpu.SemaphoreType.DMA((8,))), mib=48, flops=10**8,
    )(x)
    block, k4t = call(start_body, [((320, 128), F32), ((64, 128), F32)], (VMEM,) * 5, mib=12, flops=10**9)(
        high, low, factor_init.T, factor_four.T, factor_two
    )
    block = trade(block.reshape(8, 40, 128), ROW)
    block, whole_two, twice = call(
        second_body, [((256, 128), F32), ((64, 32), F32), ((64, 64), F32)], (VMEM, VMEM), flops=10**7
    )(block, factor_three)
    block = trade(block.reshape(32, 8, 128), COL)
    (block,) = call(third_body, [((128, 128), F32)], (VMEM,), flops=10**7)(block.reshape(256, 128))
    block = trade(block.reshape(32, 4, 128), COL)
    (block,) = call(back_body, [((8, 32, 128), F32)], (VMEM, VMEM), flops=10**7)(block.reshape(128, 128), whole_two)
    block = trade(block, ROW)
    (image,) = call(image_body, [((512, 128), F32)], (VMEM,) * 4, mib=12, flops=10**9)(
        block.reshape(256, 128), k4t, high, low
    )
    image = trade(image.reshape(32, 16, 128), PLANE)
    (image,) = call(sum_body, [((8, 16, 128), F32)], (VMEM,), flops=10**6)(image)
    image = trade(image, "z")
    (image,) = call(sum_body, [((32, 16, 128), F32)], (VMEM,), flops=10**6)(image)
    image = trade(image, PLANE)
    block, turned = call(
        core_two_body, [((256, 128), F32), ((64, 1024), F32)], (VMEM,) * 4, mib=12, flops=10**9
    )(image.reshape(512, 128), high, low, k4t)
    block = trade(block.reshape(8, 32, 128), ROW)
    square = mm(turned, turned, 1, 1)
    lower = jnp.linalg.cholesky(square)
    linv = jax.scipy.linalg.solve_triangular(lower, jnp.eye(64, dtype=F32), lower=True)
    basis = mm(linv, turned)
    (block,) = call(core_three_body, [((1024, 128), F32)], (VMEM, VMEM, SMEM), flops=10**7)(block, twice, factor_three)
    block = trade(block.reshape(256, 4, 128), ROW + COL)
    (core,) = call(core_body, [((64, 64), F32)], (VMEM, VMEM), scratch=(pltpu.VMEM((64, 128), F32),), flops=10**7)(
        block.reshape(1024, 128), linv
    )
    return basis.T, core.reshape(4, 1, 16, 64).transpose(3, 0, 1, 2)


def solution(mesh):
    split = Mesh(mesh.devices.reshape(4, 2, 4, 8), ("x", "k", "y", "z"))
    in_specs = (P(None, ROW, COL), P(ROW, None), P(COL, None), P(), P())
    out_specs = (P(), P(None, ROW, COL, None))
    return jax.shard_map(shards, mesh=split, in_specs=in_specs, out_specs=out_specs, check_vma=False)
```

```python
import jax
import jax.numpy as jnp
from jax import lax
from jax.experimental import pallas as pl
from jax.experimental.pallas import tpu as pltpu
from jax.sharding import Mesh
from jax.sharding import PartitionSpec as P

ROW = ("x", "k")
COL = ("y", "z")
PLANE = ("x", "k", "y")
F32 = jnp.float32
BF16 = jnp.bfloat16
HBM = pltpu.HBM
VMEM = pltpu.VMEM
SMEM = pltpu.SMEM


def mm(a, b, left=1, right=0):
    return lax.dot_general(
        a, b, (((left,), (right,)), ((), ())),
        precision=lax.Precision.HIGHEST, preferred_element_type=F32,
    )


def mm16(a, b):
    return jnp.dot(a, b, preferred_element_type=F32)


def halves(a):
    high = a.astype(BF16)
    return high, (a - high.astype(F32)).astype(BF16)


def call(body, outs, spaces, scratch=(), mib=4, flops=0):
    vmem = pl.BlockSpec(memory_space=pltpu.VMEM)
    specs = [pl.BlockSpec(memory_space=s) for s in spaces]
    return pl.pallas_call(
        body,
        out_shape=[jax.ShapeDtypeStruct(s, d) for s, d in outs],
        in_specs=specs,
        out_specs=[vmem] * len(outs),
        scratch_shapes=list(scratch),
        compiler_params=pltpu.CompilerParams(vmem_limit_bytes=mib << 20),
        cost_estimate=pl.CostEstimate(flops=flops, bytes_accessed=1 << 20, transcendentals=0),
    )


def fourth_matrix(f4t):
    wide = jnp.concatenate([f4t] * 4, axis=1)
    owner = lax.broadcasted_iota(jnp.int32, (8, 128), 1) // 32
    rows = [
        jnp.where(owner == c, wide[lo * 8 : lo * 8 + 8], 0.0) for lo in range(2) for c in range(4)
    ]
    return jnp.concatenate(rows, axis=0)


def fourth_mode(z, k4t):
    stack = jnp.concatenate([z[:, b * 128 : (b + 1) * 128] for b in range(8)], axis=0)
    m = mm(k4t, stack, 1, 1)
    return [
        jnp.concatenate([m[:32, b * 64 : b * 64 + 64], m[32:, b * 64 : b * 64 + 64]], axis=1)
        for b in range(8)
    ]


def split_body(x_ref, high_ref, low_ref, held, sems):
    def copy(i):
        part = pl.ds(i * 1024, 1024)
        return pltpu.make_async_copy(x_ref.at[part], held.at[part], sems.at[i])

    for i in range(8):
        copy(i).start()
    for i in range(8):
        copy(i).wait()
        rows = slice(i * 128, i * 128 + 128)
        for b in range(8):
            high, low = halves(held[pl.ds(i * 1024 + b, 128, stride=8), :])
            high_ref[rows, b * 128 : b * 128 + 128] = high
            low_ref[rows, b * 128 : b * 128 + 128] = low


def first_mode(bt, high_ref, low_ref):
    bt_high, bt_low = halves(bt)
    major = mm16(jnp.concatenate([bt_high, bt_low], axis=0), high_ref[...])
    return major[:64] + major[64:] + mm16(bt_high, low_ref[...])


def start_body(high_ref, low_ref, bt_ref, f4t_ref, f2_ref, out_ref):
    k4t = fourth_matrix(f4t_ref[...])
    tail = jnp.concatenate([f2_ref[...], jnp.zeros((8, 96), F32)], axis=1)
    for i in range(8):
        out_ref[i * 40 + 32 : i * 40 + 40, :] = tail
    z = first_mode(bt_ref[...], high_ref, low_ref)
    for b, comb in enumerate(fourth_mode(z, k4t)):
        for c in range(4):
            out_ref[pl.ds(c * 8 + b, 8, stride=40), :] = comb[c * 8 : (c + 1) * 8]


def pack_body(high_ref, low_ref, f4t_ref, me_ref, *refs):
    outs, (mat_high, mat_low) = refs[:8], refs[8:]
    lane = lax.broadcasted_iota(jnp.int32, (16, 512), 1)
    index = lax.broadcasted_iota(jnp.int32, (16, 512), 0)
    owner = lane // 8 % 2 * 8 + (me_ref[0] + lane // 64) % 8
    wide = mm(f4t_ref[...], jnp.where(index == owner, 1.0, 0.0).astype(F32), 0, 0)
    lane = lax.broadcasted_iota(jnp.int32, (32, 512), 1)
    spot = lane % 8 * 4 + lane // 16 % 4
    wide_high, wide_low = halves(wide)
    for n in range(32):
        mat_high[n * 32 : n * 32 + 32, :] = jnp.where(spot == n, wide_high.astype(F32), 0.0).astype(BF16)
        mat_low[n * 32 : n * 32 + 32, :] = jnp.where(spot == n, wide_low.astype(F32), 0.0).astype(BF16)
    for t in range(4):
        parts = []
        for start in (t * 128, 512 + t * 128):
            rows = slice(start, start + 128)
            parts.append(
                mm16(high_ref[rows, :], mat_high[...])
                + mm16(high_ref[rows, :], mat_low[...])
                + mm16(low_ref[rows, :], mat_high[...])
            )
        for n, out in enumerate(outs):
            lanes = slice(n * 64, n * 64 + 64)
            out[t * 128 : t * 128 + 128, :] = jnp.concatenate([p[:, lanes] for p in parts], axis=1)


def second_body(r_ref, f3_ref, me_ref, out_ref, f2_ref, twice_ref):
    f2 = r_ref[:, 32:40, :].reshape(64, 128)[:, :32]
    data = jnp.concatenate([r_ref[:, c * 8 : (c + 1) * 8, :].reshape(64, 128) for c in range(4)], axis=1)
    y = mm(f2, data, 0, 0)
    f3 = jnp.concatenate([f3_ref[...], jnp.zeros((4, 96), F32)], axis=1)
    for c in range(4):
        out_ref[pl.ds(c, 32, stride=8), :] = y[:, c * 128 : (c + 1) * 128]
        out_ref[pl.ds(4 + c, 32, stride=8), :] = jnp.broadcast_to(f3[c : c + 1], (32, 128))
    turned = jnp.concatenate([r_ref[(me_ref[0] - t + 8) % 8, 32:40, :] for t in range(8)], axis=0)[:, :32]
    f2_ref[...] = turned
    g = lax.broadcasted_iota(jnp.int32, (32, 64), 0)
    slot = lax.broadcasted_iota(jnp.int32, (32, 64), 1)
    twice_ref[...] = mm(turned, jnp.where(slot // 8 * 4 + slot % 4 == g, 1.0, 0.0).astype(F32))


def third_body(r_ref, out_ref):
    data = jnp.concatenate([r_ref[pl.ds(c, 32, stride=8), :] for c in range(4)], axis=0)
    f3 = jnp.concatenate([r_ref[pl.ds(4 + c, 32, stride=8), :] for c in range(4)], axis=0)[:, :32]
    q = mm(f3, mm(f3, data, 0, 0))
    for c in range(4):
        out_ref[pl.ds(c, 32, stride=4), :] = q[c * 32 : (c + 1) * 32]


def image_body(r_ref, f2_ref, *refs):
    blocks, (out_ref, high_ref, low_ref) = refs[:8], refs[8:]
    for t, block in enumerate(blocks):
        lanes = slice(t * 128, t * 128 + 128)
        high_ref[:, lanes], low_ref[:, lanes] = halves(block[...])
    data = jnp.concatenate([r_ref[pl.ds(c, 32, stride=4), :] for c in range(4)], axis=1)
    y = mm(f2_ref[...], data)
    zero = jnp.zeros((64, 64), F32)
    rows = []
    for t in range(8):
        w = jnp.concatenate([y[t * 8 : t * 8 + 8, n * 64 : n * 64 + 64] for n in range(8)], axis=0)
        rows += [jnp.concatenate([w, zero], axis=1), jnp.concatenate([zero, w], axis=1)]
    w_high, w_low = halves(jnp.concatenate(rows, axis=0))
    out_ref[...] = mm16(high_ref[...], w_high) + mm16(high_ref[...], w_low) + mm16(low_ref[...], w_high)


def sum_body(r_ref, out_ref):
    total = r_ref[0]
    for i in range(1, r_ref.shape[0]):
        total = total + r_ref[i]
    for i in range(out_ref.shape[0]):
        out_ref[i] = total


def core_two_body(image_ref, high_ref, low_ref, twice_ref, f3_ref, out_ref, turned_ref):
    flat = image_ref[...].T
    turned_ref[...] = jnp.concatenate([flat[:64], flat[64:]], axis=1)
    bt_high, bt_low = halves(flat)
    z = mm16(jnp.concatenate([bt_high, bt_low], axis=0), high_ref[...])
    z = z[:128] + z[128:] + mm16(bt_high, low_ref[...])
    z = jnp.concatenate(
        [z[:64, t * 128 : t * 128 + 64] + z[64:, t * 128 + 64 : t * 128 + 128] for t in range(8)], axis=1
    ).T
    pieces = [
        jnp.concatenate([z[t * 64 + n * 8 : t * 64 + n * 8 + 8] for t in range(8)], axis=0) for n in range(8)
    ]
    y = mm(twice_ref[...], jnp.concatenate(pieces, axis=1), 0, 0)
    upper = lax.broadcasted_iota(jnp.int32, (8, 128), 0) < 4
    for f in range(0, 32, 2):
        scale = [jnp.where(upper, f3_ref[c, f], f3_ref[c, f + 1]) for c in range(4)]
        for i in range(8):
            piece = scale[0] * y[i * 8 : i * 8 + 8, :128]
            for c in range(1, 4):
                piece = piece + scale[c] * y[i * 8 : i * 8 + 8, c * 128 : c * 128 + 128]
            out_ref[(i * 32 + f) * 4 : (i * 32 + f) * 4 + 8, :] = piece


def core_body(r_ref, linv_ref, out_ref, kept):
    for i in range(8):
        total = r_ref[i * 128 : i * 128 + 8, :]
        for t in range(1, 16):
            total = total + r_ref[i * 128 + t * 8 : i * 128 + t * 8 + 8, :]
        kept[i * 8 : i * 8 + 8, :] = total + pltpu.roll(total, 4, 0)
    parts = []
    for g in range(4):
        tile = kept[pl.ds(g, 8, stride=8), :]
        parts += [tile[:, :64], tile[:, 64:]]
    out_ref[...] = mm(jnp.concatenate(parts, axis=0), linv_ref[...], 1, 1)


def trade(block, axis):
    return lax.all_to_all(block, axis, split_axis=0, concat_axis=0, tiled=True)


def shards(tensor, factor_two, factor_three, factor_four, factor_init):
    x = tensor.reshape(8192, 128)
    high, low = call(
        split_body, [((1024, 1024), BF16)] * 2, (HBM,),
        scratch=(pltpu.VMEM((8192, 128), F32), pltpu.SemaphoreType.DMA((8,))), mib=48, flops=10**8,
    )(x)
    me = lax.axis_index(ROW).astype(jnp.int32).reshape(1)
    (block,) = call(start_body, [((320, 128), F32)], (VMEM,) * 5, mib=12, flops=10**9)(
        high, low, factor_init.T, factor_four.T, factor_two
    )
    blocks = call(
        pack_body, [((512, 128), F32)] * 8, (VMEM,) * 3 + (SMEM,),
        scratch=(pltpu.VMEM((1024, 512), BF16),) * 2, mib=16, flops=3 * 10**9,
    )(high, low, factor_four.T, me)
    block = trade(block.reshape(8, 40, 128), ROW)
    block, f2, twice = call(
        second_body, [((256, 128), F32), ((64, 32), F32), ((64, 64), F32)], (VMEM, VMEM, SMEM), flops=10**7
    )(block, factor_three, me)
    blocks = [blocks[0]] + [
        lax.ppermute(blocks[t], ROW, [(i, (i + t) % 8) for i in range(8)]) for t in range(1, 8)
    ]
    block = trade(block.reshape(32, 8, 128), COL)
    (block,) = call(third_body, [((128, 128), F32)], (VMEM,), flops=10**7)(block.reshape(256, 128))
    block = trade(block.reshape(32, 4, 128), COL)
    image, high, low = call(
        image_body, [((512, 128), F32), ((512, 1024), BF16), ((512, 1024), BF16)], (VMEM,) * 10, mib=12, flops=10**9
    )(block.reshape(128, 128), f2, *blocks)
    image = trade(image.reshape(32, 16, 128), PLANE)
    (image,) = call(sum_body, [((8, 16, 128), F32)], (VMEM,), flops=10**6)(image)
    image = trade(image, "z")
    (image,) = call(sum_body, [((32, 16, 128), F32)], (VMEM,), flops=10**6)(image)
    image = trade(image, PLANE)
    block, turned = call(
        core_two_body, [((1024, 128), F32), ((64, 1024), F32)], (VMEM,) * 4 + (SMEM,), mib=12, flops=10**9
    )(image.reshape(512, 128), high, low, twice, factor_three)
    square = mm(turned, turned, 1, 1)
    lower = jnp.linalg.cholesky(square)
    linv = jax.scipy.linalg.solve_triangular(lower, jnp.eye(64, dtype=F32), lower=True)
    basis = mm(linv, turned)
    block = trade(block.reshape(256, 4, 128), ROW + COL)
    (core,) = call(core_body, [((64, 64), F32)], (VMEM, VMEM), scratch=(pltpu.VMEM((64, 128), F32),), flops=10**7)(
        block.reshape(1024, 128), linv
    )
    return basis.T, core.reshape(4, 1, 16, 64).transpose(3, 0, 1, 2)


def solution(mesh):
    split = Mesh(mesh.devices.reshape(4, 2, 4, 8), ("x", "k", "y", "z"))
    in_specs = (P(None, ROW, COL), P(ROW, None), P(COL, None), P(), P())
    out_specs = (P(), P(None, ROW, COL, None))
    return jax.shard_map(shards, mesh=split, in_specs=in_specs, out_specs=out_specs, check_vma=False)
```

```python
import jax
import jax.numpy as jnp
from jax import lax
from jax.experimental import pallas as pl
from jax.experimental.pallas import tpu as pltpu
from jax.sharding import Mesh
from jax.sharding import PartitionSpec as P


ROW = ("x", "k")
COL = ("y", "z")
PLANE = ("x", "k", "y")
F32 = jnp.float32
BF16 = jnp.bfloat16
HBM = pltpu.HBM
VMEM = pltpu.VMEM
SMEM = pltpu.SMEM


def mm(a, b, left=1, right=0):
    return lax.dot_general(
        a, b, (((left,), (right,)), ((), ())),
        precision=lax.Precision.HIGHEST, preferred_element_type=F32,
    )


def mm16(a, b):
    return jnp.dot(a, b, preferred_element_type=F32)


def halves(a):
    high = a.astype(BF16)
    return high, (a - high.astype(F32)).astype(BF16)


def call(body, outs, spaces, scratch=(), mib=4, flops=0):
    vmem = pl.BlockSpec(memory_space=pltpu.VMEM)
    specs = [pl.BlockSpec(memory_space=s) for s in spaces]
    return pl.pallas_call(
        body,
        out_shape=[jax.ShapeDtypeStruct(s, d) for s, d in outs],
        in_specs=specs,
        out_specs=[vmem] * len(outs),
        scratch_shapes=list(scratch),
        compiler_params=pltpu.CompilerParams(vmem_limit_bytes=mib << 20),
        cost_estimate=pl.CostEstimate(flops=flops, bytes_accessed=1 << 20, transcendentals=0),
    )


def fourth_matrix(f4t):
    wide = jnp.concatenate([f4t] * 4, axis=1)
    owner = lax.broadcasted_iota(jnp.int32, (8, 128), 1) // 32
    rows = [
        jnp.where(owner == c, wide[lo * 8 : lo * 8 + 8], 0.0) for lo in range(2) for c in range(4)
    ]
    return jnp.concatenate(rows, axis=0)


def fourth_mode(z, k4t):
    stack = jnp.concatenate([z[:, b * 128 : (b + 1) * 128] for b in range(8)], axis=0)
    m = mm(k4t, stack, 1, 1)
    return [
        jnp.concatenate([m[:32, b * 64 : b * 64 + 64], m[32:, b * 64 : b * 64 + 64]], axis=1)
        for b in range(8)
    ]


def split_body(x_ref, me_ref, high_ref, low_ref, held, sems):
    del me_ref

    def copy(i):
        part = pl.ds(i * 1024, 1024)
        return pltpu.make_async_copy(x_ref.at[part], held.at[part], sems.at[i])

    for i in range(8):
        copy(i).start()
    for i in range(8):
        copy(i).wait()
        rows = slice(i * 128, i * 128 + 128)
        for b in range(8):
            high, low = halves(held[pl.ds(i * 1024 + b, 128, stride=8), :])
            high_ref[rows, b * 128 : b * 128 + 128] = high
            low_ref[rows, b * 128 : b * 128 + 128] = low


def first_mode(bt, high_ref, low_ref):
    bt_high, bt_low = halves(bt)
    major = mm16(jnp.concatenate([bt_high, bt_low], axis=0), high_ref[...])
    return major[:64] + major[64:] + mm16(bt_high, low_ref[...])


def start_body(high_ref, low_ref, bt_ref, f4t_ref, f2_ref, own_ref, out_ref):
    del own_ref
    k4t = fourth_matrix(f4t_ref[...])
    tail = jnp.concatenate([f2_ref[...], jnp.zeros((8, 96), F32)], axis=1)
    for i in range(8):
        out_ref[i * 40 + 32 : i * 40 + 40, :] = tail
    z = first_mode(bt_ref[...], high_ref, low_ref)
    for b, comb in enumerate(fourth_mode(z, k4t)):
        for c in range(4):
            out_ref[pl.ds(c * 8 + b, 8, stride=40), :] = comb[c * 8 : (c + 1) * 8]


def pack_body(high_ref, low_ref, f4t_ref, me_ref, *refs):
    outs, (mat_high, mat_low) = refs[:8], refs[8:]
    lane = lax.broadcasted_iota(jnp.int32, (16, 512), 1)
    index = lax.broadcasted_iota(jnp.int32, (16, 512), 0)
    owner = lane // 8 % 2 * 8 + (me_ref[0] + lane // 64) % 8
    wide = mm(f4t_ref[...], jnp.where(index == owner, 1.0, 0.0).astype(F32), 0, 0)
    lane = lax.broadcasted_iota(jnp.int32, (32, 512), 1)
    spot = lane % 8 * 4 + lane // 16 % 4
    wide_high, wide_low = halves(wide)
    for n in range(32):
        mat_high[n * 32 : n * 32 + 32, :] = jnp.where(spot == n, wide_high.astype(F32), 0.0).astype(BF16)
        mat_low[n * 32 : n * 32 + 32, :] = jnp.where(spot == n, wide_low.astype(F32), 0.0).astype(BF16)
    for t in range(4):
        parts = []
        for start in (t * 128, 512 + t * 128):
            rows = slice(start, start + 128)
            parts.append(
                mm16(high_ref[rows, :], mat_high[...])
                + mm16(high_ref[rows, :], mat_low[...])
                + mm16(low_ref[rows, :], mat_high[...])
            )
        for n, out in enumerate(outs):
            lanes = slice(n * 64, n * 64 + 64)
            out[t * 128 : t * 128 + 128, :] = jnp.concatenate([p[:, lanes] for p in parts], axis=1)


def second_body(r_ref, f3_ref, me_ref, out_ref, f2_ref, twice_ref):
    f2 = r_ref[:, 32:40, :].reshape(64, 128)[:, :32]
    data = jnp.concatenate([r_ref[:, c * 8 : (c + 1) * 8, :].reshape(64, 128) for c in range(4)], axis=1)
    y = mm(f2, data, 0, 0)
    f3 = jnp.concatenate([f3_ref[...], jnp.zeros((4, 96), F32)], axis=1)
    for c in range(4):
        out_ref[pl.ds(c, 32, stride=8), :] = y[:, c * 128 : (c + 1) * 128]
        out_ref[pl.ds(4 + c, 32, stride=8), :] = jnp.broadcast_to(f3[c : c + 1], (32, 128))
    turned = jnp.concatenate([r_ref[(me_ref[0] - t + 8) % 8, 32:40, :] for t in range(8)], axis=0)[:, :32]
    f2_ref[...] = turned
    g = lax.broadcasted_iota(jnp.int32, (32, 64), 0)
    slot = lax.broadcasted_iota(jnp.int32, (32, 64), 1)
    twice_ref[...] = mm(turned, jnp.where(slot // 8 * 4 + slot % 4 == g, 1.0, 0.0).astype(F32))


def third_body(r_ref, out_ref):
    data = jnp.concatenate([r_ref[pl.ds(c, 32, stride=8), :] for c in range(4)], axis=0)
    f3 = jnp.concatenate([r_ref[pl.ds(4 + c, 32, stride=8), :] for c in range(4)], axis=0)[:, :32]
    q = mm(f3, mm(f3, data, 0, 0))
    for c in range(4):
        out_ref[pl.ds(c, 32, stride=4), :] = q[c * 32 : (c + 1) * 32]


def image_body(r_ref, f2_ref, *refs):
    blocks, (out_ref, high_ref, low_ref) = refs[:8], refs[8:]
    for t, block in enumerate(blocks):
        lanes = slice(t * 128, t * 128 + 128)
        high_ref[:, lanes], low_ref[:, lanes] = halves(block[...])
    data = jnp.concatenate([r_ref[pl.ds(c, 32, stride=4), :] for c in range(4)], axis=1)
    y = mm(f2_ref[...], data)
    zero = jnp.zeros((64, 64), F32)
    rows = []
    for t in range(8):
        w = jnp.concatenate([y[t * 8 : t * 8 + 8, n * 64 : n * 64 + 64] for n in range(8)], axis=0)
        rows += [jnp.concatenate([w, zero], axis=1), jnp.concatenate([zero, w], axis=1)]
    w_high, w_low = halves(jnp.concatenate(rows, axis=0))
    out_ref[...] = mm16(high_ref[...], w_high) + mm16(high_ref[...], w_low) + mm16(low_ref[...], w_high)


def sum_body(r_ref, out_ref):
    total = r_ref[0]
    for i in range(1, r_ref.shape[0]):
        total = total + r_ref[i]
    for i in range(out_ref.shape[0]):
        out_ref[i] = total


def core_two_body(image_ref, high_ref, low_ref, twice_ref, f3_ref, out_ref, turned_ref):
    flat = image_ref[...].T
    turned_ref[...] = jnp.concatenate([flat[:64], flat[64:]], axis=1)
    bt_high, bt_low = halves(flat)
    z = mm16(jnp.concatenate([bt_high, bt_low], axis=0), high_ref[...])
    z = z[:128] + z[128:] + mm16(bt_high, low_ref[...])
    z = jnp.concatenate(
        [z[:64, t * 128 : t * 128 + 64] + z[64:, t * 128 + 64 : t * 128 + 128] for t in range(8)], axis=1
    ).T
    pieces = [
        jnp.concatenate([z[t * 64 + n * 8 : t * 64 + n * 8 + 8] for t in range(8)], axis=0) for n in range(8)
    ]
    y = mm(twice_ref[...], jnp.concatenate(pieces, axis=1), 0, 0)
    upper = lax.broadcasted_iota(jnp.int32, (8, 128), 0) < 4
    for f in range(0, 32, 2):
        scale = [jnp.where(upper, f3_ref[c, f], f3_ref[c, f + 1]) for c in range(4)]
        for i in range(8):
            piece = scale[0] * y[i * 8 : i * 8 + 8, :128]
            for c in range(1, 4):
                piece = piece + scale[c] * y[i * 8 : i * 8 + 8, c * 128 : c * 128 + 128]
            out_ref[(i * 32 + f) * 4 : (i * 32 + f) * 4 + 8, :] = piece


def core_body(r_ref, linv_ref, out_ref, kept):
    for i in range(8):
        total = r_ref[i * 128 : i * 128 + 8, :]
        for t in range(1, 16):
            total = total + r_ref[i * 128 + t * 8 : i * 128 + t * 8 + 8, :]
        kept[i * 8 : i * 8 + 8, :] = total + pltpu.roll(total, 4, 0)
    parts = []
    for g in range(4):
        tile = kept[pl.ds(g, 8, stride=8), :]
        parts += [tile[:, :64], tile[:, 64:]]
    out_ref[...] = mm(jnp.concatenate(parts, axis=0), linv_ref[...], 1, 1)


def turn(block, t):
    return lax.ppermute(block, ROW, [(i, (i + t) % 8) for i in range(8)])


def trade(block, axis):
    return lax.all_to_all(block, axis, split_axis=0, concat_axis=0, tiled=True)


def shards(tensor, factor_two, factor_three, factor_four, factor_init):
    x = tensor.reshape(8192, 128)
    me = lax.axis_index(ROW).astype(jnp.int32).reshape(1)
    high, low = call(
        split_body, [((1024, 1024), BF16)] * 2, (HBM, SMEM),
        scratch=(pltpu.VMEM((8192, 128), F32), pltpu.SemaphoreType.DMA((8,))), mib=48, flops=10**8,
    )(x, me)
    blocks = call(
        pack_body, [((512, 128), F32)] * 8, (VMEM,) * 3 + (SMEM,),
        scratch=(pltpu.VMEM((1024, 512), BF16),) * 2, mib=16, flops=3 * 10**9,
    )(high, low, factor_four.T, me)
    (block,) = call(start_body, [((320, 128), F32)], (VMEM,) * 6, mib=12, flops=10**9)(
        high, low, factor_init.T, factor_four.T, factor_two, blocks[0]
    )
    block = trade(block.reshape(8, 40, 128), ROW)
    block, f2, twice = call(
        second_body, [((256, 128), F32), ((64, 32), F32), ((64, 64), F32)], (VMEM, VMEM, SMEM), flops=10**7
    )(block, factor_three, me)
    blocks = [blocks[0]] + [turn(blocks[t], t) for t in range(1, 8)]
    block = trade(block.reshape(32, 8, 128), COL)
    (block,) = call(third_body, [((128, 128), F32)], (VMEM,), flops=10**7)(block.reshape(256, 128))
    block = trade(block.reshape(32, 4, 128), COL)
    image, high, low = call(
        image_body, [((512, 128), F32), ((512, 1024), BF16), ((512, 1024), BF16)], (VMEM,) * 10, mib=12, flops=10**9
    )(block.reshape(128, 128), f2, *blocks)
    image = trade(image.reshape(32, 16, 128), PLANE)
    (image,) = call(sum_body, [((8, 16, 128), F32)], (VMEM,), flops=10**6)(image)
    image = trade(image, "z")
    (image,) = call(sum_body, [((32, 16, 128), F32)], (VMEM,), flops=10**6)(image)
    image = trade(image, PLANE)
    block, turned = call(
        core_two_body, [((1024, 128), F32), ((64, 1024), F32)], (VMEM,) * 4 + (SMEM,), mib=12, flops=10**9
    )(image.reshape(512, 128), high, low, twice, factor_three)
    square = mm(turned, turned, 1, 1)
    lower = jnp.linalg.cholesky(square)
    linv = jax.scipy.linalg.solve_triangular(lower, jnp.eye(64, dtype=F32), lower=True)
    basis = mm(linv, turned)
    block = trade(block.reshape(256, 4, 128), ROW + COL)
    (core,) = call(core_body, [((64, 64), F32)], (VMEM, VMEM), scratch=(pltpu.VMEM((64, 128), F32),), flops=10**7)(
        block.reshape(1024, 128), linv
    )
    return basis.T, core.reshape(4, 1, 16, 64).transpose(3, 0, 1, 2)


def solution(mesh):
    split = Mesh(mesh.devices.reshape(4, 2, 4, 8), ("x", "k", "y", "z"))
    in_specs = (P(None, ROW, COL), P(ROW, None), P(COL, None), P(), P())
    out_specs = (P(), P(None, ROW, COL, None))
    return jax.shard_map(shards, mesh=split, in_specs=in_specs, out_specs=out_specs, check_vma=False)
```

```python
import jax
import jax.numpy as jnp
from jax import lax
from jax.experimental import pallas as pl
from jax.experimental.pallas import tpu as pltpu
from jax.sharding import Mesh
from jax.sharding import PartitionSpec as P


ROW = ("x", "k")
COL = ("y", "z")
PLANE = ("x", "k", "y")
F32 = jnp.float32
BF16 = jnp.bfloat16
HBM = pltpu.HBM
VMEM = pltpu.VMEM
SMEM = pltpu.SMEM


def mm(a, b, left=1, right=0):
    return lax.dot_general(
        a, b, (((left,), (right,)), ((), ())),
        precision=lax.Precision.HIGHEST, preferred_element_type=F32,
    )


def mm16(a, b):
    return jnp.dot(a, b, preferred_element_type=F32)


def halves(a):
    high = a.astype(BF16)
    return high, (a - high.astype(F32)).astype(BF16)


def call(body, outs, spaces, scratch=(), mib=4, flops=0):
    vmem = pl.BlockSpec(memory_space=pltpu.VMEM)
    specs = [pl.BlockSpec(memory_space=s) for s in spaces]
    return pl.pallas_call(
        body,
        out_shape=[jax.ShapeDtypeStruct(s, d) for s, d in outs],
        in_specs=specs,
        out_specs=[vmem] * len(outs),
        scratch_shapes=list(scratch),
        compiler_params=pltpu.CompilerParams(vmem_limit_bytes=mib << 20),
        cost_estimate=pl.CostEstimate(flops=flops, bytes_accessed=1 << 20, transcendentals=0),
    )


def split_body(x_ref, me_ref, high_ref, low_ref, held, sems):
    del me_ref

    def copy(i):
        part = pl.ds(i * 1024, 1024)
        return pltpu.make_async_copy(x_ref.at[part], held.at[part], sems.at[i])

    for i in range(8):
        copy(i).start()
    for i in range(8):
        copy(i).wait()
        rows = slice(i * 128, i * 128 + 128)
        for b in range(8):
            high, low = halves(held[pl.ds(i * 1024 + b, 128, stride=8), :])
            high_ref[rows, b * 128 : b * 128 + 128] = high
            low_ref[rows, b * 128 : b * 128 + 128] = low


def pack_body(high_ref, low_ref, f4t_ref, bt_ref, f2_ref, me_ref, *refs):
    outs, (first_ref, mat_high, mat_low) = refs[:8], refs[8:]
    lane = lax.broadcasted_iota(jnp.int32, (16, 512), 1)
    index = lax.broadcasted_iota(jnp.int32, (16, 512), 0)
    owner = lane // 8 % 2 * 8 + (me_ref[0] + lane // 64) % 8
    wide = mm(f4t_ref[...], jnp.where(index == owner, 1.0, 0.0).astype(F32), 0, 0)
    lane = lax.broadcasted_iota(jnp.int32, (32, 512), 1)
    spot = lane % 8 * 4 + lane // 16 % 4
    wide_high, wide_low = halves(wide)
    for n in range(32):
        mat_high[n * 32 : n * 32 + 32, :] = jnp.where(spot == n, wide_high.astype(F32), 0.0).astype(BF16)
        mat_low[n * 32 : n * 32 + 32, :] = jnp.where(spot == n, wide_low.astype(F32), 0.0).astype(BF16)
    bt_high, bt_low = halves(bt_ref[...])
    both = jnp.concatenate([bt_high, bt_low], axis=0)
    tail = jnp.concatenate([f2_ref[...], jnp.zeros((8, 96), F32)], axis=1)
    for i in range(8):
        first_ref[i, 32:40, :] = tail
    z = jnp.zeros((64, 512), F32)
    for t in range(4):
        parts = []
        spans = [slice(start, start + 128) for start in (t * 128, 512 + t * 128)]
        for rows in spans:
            parts.append(
                mm16(high_ref[rows, :], mat_high[...])
                + mm16(high_ref[rows, :], mat_low[...])
                + mm16(low_ref[rows, :], mat_high[...])
            )
        for n, out in enumerate(outs):
            lanes = slice(n * 64, n * 64 + 64)
            out[t * 128 : t * 128 + 128, :] = jnp.concatenate([p[:, lanes] for p in parts], axis=1)
        p_high, p_low = halves(jnp.concatenate(parts, axis=0))
        major = mm16(jnp.concatenate([both[:, rows] for rows in spans], axis=1), p_high)
        z = z + major[:64] + major[64:] + mm16(jnp.concatenate([bt_high[:, rows] for rows in spans], axis=1), p_low)
    z = z.T
    for n in range(8):
        for c in range(4):
            base = n * 64 + c * 16
            first_ref[(me_ref[0] + n) % 8, c * 8 : c * 8 + 8, :] = jnp.concatenate(
                [z[base : base + 8], z[base + 8 : base + 16]], axis=1
            )


def second_body(r_ref, f3_ref, me_ref, out_ref, f2_ref):
    f2 = r_ref[:, 32:40, :].reshape(64, 128)[:, :32]
    data = jnp.concatenate([r_ref[:, c * 8 : (c + 1) * 8, :].reshape(64, 128) for c in range(4)], axis=1)
    y = mm(f2, data, 0, 0)
    f3 = jnp.concatenate([f3_ref[c : c + 1, :] for c in range(4)], axis=1)
    for c in range(4):
        out_ref[pl.ds(c, 32, stride=5), :] = y[:, c * 128 : (c + 1) * 128]
    out_ref[pl.ds(4, 32, stride=5), :] = jnp.broadcast_to(f3, (32, 128))
    turned = jnp.concatenate([r_ref[(me_ref[0] - t + 8) % 8, 32:40, :] for t in range(8)], axis=0)[:, :32]
    f2_ref[...] = turned


def third_body(r_ref, out_ref):
    data = jnp.concatenate([r_ref[pl.ds(c, 32, stride=5), :] for c in range(4)], axis=0)
    f3 = r_ref[pl.ds(4, 32, stride=5), :]
    f3 = jnp.concatenate([f3[:, c * 32 : c * 32 + 32] for c in range(4)], axis=0)
    q = mm(f3, mm(f3, data, 0, 0))
    for c in range(4):
        out_ref[pl.ds(c, 32, stride=4), :] = q[c * 32 : (c + 1) * 32]


def image_body(r_ref, f2_ref, *refs):
    blocks, (out_ref, high_ref, low_ref) = refs[:8], refs[8:]
    for t, block in enumerate(blocks):
        lanes = slice(t * 128, t * 128 + 128)
        high_ref[:, lanes], low_ref[:, lanes] = halves(block[...])
    data = jnp.concatenate([r_ref[pl.ds(c, 32, stride=4), :] for c in range(4)], axis=1)
    y = mm(f2_ref[...], data)
    zero = jnp.zeros((64, 64), F32)
    rows = []
    for t in range(8):
        w = jnp.concatenate([y[t * 8 : t * 8 + 8, n * 64 : n * 64 + 64] for n in range(8)], axis=0)
        rows += [jnp.concatenate([w, zero], axis=1), jnp.concatenate([zero, w], axis=1)]
    w_high, w_low = halves(jnp.concatenate(rows, axis=0))
    out_ref[...] = mm16(high_ref[...], w_high) + mm16(high_ref[...], w_low) + mm16(low_ref[...], w_high)


def sum_body(r_ref, out_ref):
    total = r_ref[0]
    for i in range(1, r_ref.shape[0]):
        total = total + r_ref[i]
    for i in range(out_ref.shape[0]):
        out_ref[i] = total


def core_two_body(image_ref, high_ref, low_ref, f2_ref, f3_ref, out_ref, turned_ref):
    g = lax.broadcasted_iota(jnp.int32, (32, 64), 0)
    slot = lax.broadcasted_iota(jnp.int32, (32, 64), 1)
    twice = mm(f2_ref[...], jnp.where(slot // 8 * 4 + slot % 4 == g, 1.0, 0.0).astype(F32))
    flat = image_ref[...].T
    turned_ref[...] = jnp.concatenate([flat[:64], flat[64:]], axis=1)
    bt_high, bt_low = halves(flat)
    z = mm16(jnp.concatenate([bt_high, bt_low], axis=0), high_ref[...])
    z = z[:128] + z[128:] + mm16(bt_high, low_ref[...])
    z = jnp.concatenate(
        [z[:64, t * 128 : t * 128 + 64] + z[64:, t * 128 + 64 : t * 128 + 128] for t in range(8)], axis=1
    ).T
    pieces = [
        jnp.concatenate([z[t * 64 + n * 8 : t * 64 + n * 8 + 8] for t in range(8)], axis=0) for n in range(8)
    ]
    y = mm(twice, jnp.concatenate(pieces, axis=1), 0, 0)
    upper = lax.broadcasted_iota(jnp.int32, (8, 128), 0) < 4
    for f in range(0, 32, 2):
        scale = [jnp.where(upper, f3_ref[c, f], f3_ref[c, f + 1]) for c in range(4)]
        for i in range(8):
            piece = scale[0] * y[i * 8 : i * 8 + 8, :128]
            for c in range(1, 4):
                piece = piece + scale[c] * y[i * 8 : i * 8 + 8, c * 128 : c * 128 + 128]
            out_ref[(i * 32 + f) * 4 : (i * 32 + f) * 4 + 8, :] = piece


def core_body(r_ref, linv_ref, out_ref, kept):
    for i in range(8):
        total = r_ref[i * 128 : i * 128 + 8, :]
        for t in range(1, 16):
            total = total + r_ref[i * 128 + t * 8 : i * 128 + t * 8 + 8, :]
        kept[i * 8 : i * 8 + 8, :] = total + pltpu.roll(total, 4, 0)
    parts = []
    for g in range(4):
        tile = kept[pl.ds(g, 8, stride=8), :]
        parts += [tile[:, :64], tile[:, 64:]]
    out_ref[...] = mm(jnp.concatenate(parts, axis=0), linv_ref[...], 1, 1)


def turn(block, t):
    return lax.ppermute(block, ROW, [(i, (i + t) % 8) for i in range(8)])


def trade(block, axis):
    return lax.all_to_all(block, axis, split_axis=0, concat_axis=0, tiled=True)


def shards(tensor, factor_two, factor_three, factor_four, factor_init):
    x = tensor.reshape(8192, 128)
    me = lax.axis_index(ROW).astype(jnp.int32).reshape(1)
    high, low = call(
        split_body, [((1024, 1024), BF16)] * 2, (HBM, SMEM),
        scratch=(pltpu.VMEM((8192, 128), F32), pltpu.SemaphoreType.DMA((8,))), mib=48, flops=10**8,
    )(x, me)
    *blocks, block = call(
        pack_body, [((512, 128), F32)] * 8 + [((8, 40, 128), F32)], (VMEM,) * 5 + (SMEM,),
        scratch=(pltpu.VMEM((1024, 512), BF16),) * 2, mib=16, flops=3 * 10**9,
    )(high, low, factor_four.T, factor_init.T, factor_two, me)
    block = trade(block, ROW)
    block, f2 = call(
        second_body, [((160, 128), F32), ((64, 32), F32)], (VMEM, VMEM, SMEM), flops=10**7
    )(block, factor_three, me)
    blocks = [blocks[0]] + [turn(blocks[t], t) for t in range(1, 8)]
    block = trade(block.reshape(32, 1, 640), COL)
    (block,) = call(third_body, [((128, 128), F32)], (VMEM,), flops=10**7)(block.reshape(160, 128))
    block = trade(block.reshape(32, 4, 128), COL)
    image, high, low = call(
        image_body, [((512, 128), F32), ((512, 1024), BF16), ((512, 1024), BF16)], (VMEM,) * 10, mib=12, flops=10**9
    )(block.reshape(128, 128), f2, *blocks)
    image = trade(image.reshape(32, 16, 128), PLANE)
    (image,) = call(sum_body, [((8, 16, 128), F32)], (VMEM,), flops=10**6)(image)
    image = trade(image, "z")
    (image,) = call(sum_body, [((32, 16, 128), F32)], (VMEM,), flops=10**6)(image)
    image = trade(image, PLANE)
    block, turned = call(
        core_two_body, [((1024, 128), F32), ((64, 1024), F32)], (VMEM,) * 4 + (SMEM,), mib=12, flops=10**9
    )(image.reshape(512, 128), high, low, f2, factor_three)
    square = mm(turned, turned, 1, 1)
    lower = jnp.linalg.cholesky(square)
    linv = jax.scipy.linalg.solve_triangular(lower, jnp.eye(64, dtype=F32), lower=True)
    basis = mm(linv, turned)
    block = trade(block.reshape(256, 4, 128), ROW + COL)
    (core,) = call(core_body, [((64, 64), F32)], (VMEM, VMEM), scratch=(pltpu.VMEM((64, 128), F32),), flops=10**7)(
        block.reshape(1024, 128), linv
    )
    return basis.T, core.reshape(4, 1, 16, 64).transpose(3, 0, 1, 2)


def solution(mesh):
    split = Mesh(mesh.devices.reshape(4, 2, 4, 8), ("x", "k", "y", "z"))
    in_specs = (P(None, ROW, COL), P(ROW, None), P(COL, None), P(), P())
    out_specs = (P(), P(None, ROW, COL, None))
    return jax.shard_map(shards, mesh=split, in_specs=in_specs, out_specs=out_specs, check_vma=False)
```

```python
import jax
import jax.numpy as jnp
from jax import lax
from jax.experimental import pallas as pl
from jax.experimental.pallas import tpu as pltpu
from jax.sharding import Mesh
from jax.sharding import PartitionSpec as P


ROW = ("x", "k")
COL = ("y", "z")
PLANE = ("x", "k", "y")
F32 = jnp.float32
BF16 = jnp.bfloat16
HBM = pltpu.HBM
VMEM = pltpu.VMEM
SMEM = pltpu.SMEM


def mm(a, b, left=1, right=0):
    return lax.dot_general(
        a, b, (((left,), (right,)), ((), ())),
        precision=lax.Precision.HIGHEST, preferred_element_type=F32,
    )


def mm16(a, b):
    return jnp.dot(a, b, preferred_element_type=F32)


def halves(a):
    high = a.astype(BF16)
    return high, (a - high.astype(F32)).astype(BF16)


def call(body, outs, spaces, scratch=(), mib=4, flops=0):
    vmem = pl.BlockSpec(memory_space=pltpu.VMEM)
    specs = [pl.BlockSpec(memory_space=s) for s in spaces]
    return pl.pallas_call(
        body,
        out_shape=[jax.ShapeDtypeStruct(s, d) for s, d in outs],
        in_specs=specs,
        out_specs=[vmem] * len(outs),
        scratch_shapes=list(scratch),
        compiler_params=pltpu.CompilerParams(vmem_limit_bytes=mib << 20),
        cost_estimate=pl.CostEstimate(flops=flops, bytes_accessed=1 << 20, transcendentals=0),
    )


def split_body(x_ref, me_ref, high_ref, low_ref, held, sems):
    del me_ref

    def copy(i):
        part = pl.ds(i * 1024, 1024)
        return pltpu.make_async_copy(x_ref.at[part], held.at[part], sems.at[i])

    for i in range(8):
        copy(i).start()
    for i in range(8):
        copy(i).wait()
        rows = slice(i * 128, i * 128 + 128)
        for b in range(8):
            high, low = halves(held[pl.ds(i * 1024 + b, 128, stride=8), :])
            high_ref[rows, b * 128 : b * 128 + 128] = high
            low_ref[rows, b * 128 : b * 128 + 128] = low


def pack_body(high_ref, low_ref, f4t_ref, bt_ref, f2_ref, me_ref, *refs):
    outs, (first_ref, mat_high, mat_low) = refs[:8], refs[8:]
    lane = lax.broadcasted_iota(jnp.int32, (16, 512), 1)
    index = lax.broadcasted_iota(jnp.int32, (16, 512), 0)
    owner = lane // 8 % 2 * 8 + (me_ref[0] + lane // 64) % 8
    wide = mm(f4t_ref[...], jnp.where(index == owner, 1.0, 0.0).astype(F32), 0, 0)
    lane = lax.broadcasted_iota(jnp.int32, (32, 512), 1)
    spot = lane % 8 * 4 + lane // 16 % 4
    wide_high, wide_low = halves(wide)
    for n in range(32):
        mat_high[n * 32 : n * 32 + 32, :] = jnp.where(spot == n, wide_high.astype(F32), 0.0).astype(BF16)
        mat_low[n * 32 : n * 32 + 32, :] = jnp.where(spot == n, wide_low.astype(F32), 0.0).astype(BF16)
    bt_high, bt_low = halves(bt_ref[...])
    both = jnp.concatenate([bt_high, bt_low], axis=0)
    tail = jnp.concatenate([f2_ref[...], jnp.zeros((8, 96), F32)], axis=1)
    for i in range(8):
        first_ref[i, 32:40, :] = tail
    z = jnp.zeros((64, 512), F32)
    for t in range(2):
        parts = []
        spans = [slice(start, start + 256) for start in (t * 256, 512 + t * 256)]
        for rows in spans:
            parts.append(
                mm16(high_ref[rows, :], mat_high[...])
                + mm16(high_ref[rows, :], mat_low[...])
                + mm16(low_ref[rows, :], mat_high[...])
            )
        for n, out in enumerate(outs):
            lanes = slice(n * 64, n * 64 + 64)
            out[t * 256 : t * 256 + 256, :] = jnp.concatenate([p[:, lanes] for p in parts], axis=1)
        p_high, p_low = halves(jnp.concatenate(parts, axis=0))
        major = mm16(jnp.concatenate([both[:, rows] for rows in spans], axis=1), p_high)
        z = z + major[:64] + major[64:] + mm16(jnp.concatenate([bt_high[:, rows] for rows in spans], axis=1), p_low)
    z = z.T
    for n in range(8):
        for c in range(4):
            base = n * 64 + c * 16
            first_ref[(me_ref[0] + n) % 8, c * 8 : c * 8 + 8, :] = jnp.concatenate(
                [z[base : base + 8], z[base + 8 : base + 16]], axis=1
            )


def second_body(r_ref, f3_ref, me_ref, out_ref, f2_ref):
    f2 = r_ref[:, 32:40, :].reshape(64, 128)[:, :32]
    data = jnp.concatenate([r_ref[:, c * 8 : (c + 1) * 8, :].reshape(64, 128) for c in range(4)], axis=1)
    y = mm(f2, data, 0, 0)
    f3 = jnp.concatenate([f3_ref[c : c + 1, :] for c in range(4)], axis=1)
    for c in range(4):
        out_ref[pl.ds(c, 32, stride=5), :] = y[:, c * 128 : (c + 1) * 128]
    out_ref[pl.ds(4, 32, stride=5), :] = jnp.broadcast_to(f3, (32, 128))
    turned = jnp.concatenate([r_ref[(me_ref[0] - t + 8) % 8, 32:40, :] for t in range(8)], axis=0)[:, :32]
    f2_ref[...] = turned


def third_body(r_ref, out_ref):
    data = jnp.concatenate([r_ref[pl.ds(c, 32, stride=5), :] for c in range(4)], axis=0)
    f3 = r_ref[pl.ds(4, 32, stride=5), :]
    f3 = jnp.concatenate([f3[:, c * 32 : c * 32 + 32] for c in range(4)], axis=0)
    q = mm(f3, mm(f3, data, 0, 0))
    for c in range(4):
        out_ref[pl.ds(c, 32, stride=4), :] = q[c * 32 : (c + 1) * 32]


def image_body(r_ref, f2_ref, *refs):
    blocks, (out_ref, high_ref, low_ref) = refs[:8], refs[8:]
    for t, block in enumerate(blocks):
        lanes = slice(t * 128, t * 128 + 128)
        high_ref[:, lanes], low_ref[:, lanes] = halves(block[...])
    data = jnp.concatenate([r_ref[pl.ds(c, 32, stride=4), :] for c in range(4)], axis=1)
    y = mm(f2_ref[...], data)
    zero = jnp.zeros((64, 64), F32)
    rows = []
    for t in range(8):
        w = jnp.concatenate([y[t * 8 : t * 8 + 8, n * 64 : n * 64 + 64] for n in range(8)], axis=0)
        rows += [jnp.concatenate([w, zero], axis=1), jnp.concatenate([zero, w], axis=1)]
    w_high, w_low = halves(jnp.concatenate(rows, axis=0))
    out_ref[...] = mm16(high_ref[...], w_high) + mm16(high_ref[...], w_low) + mm16(low_ref[...], w_high)


def sum_body(r_ref, out_ref):
    total = r_ref[0]
    for i in range(1, r_ref.shape[0]):
        total = total + r_ref[i]
    for i in range(out_ref.shape[0]):
        out_ref[i] = total


def core_two_body(image_ref, high_ref, low_ref, f2_ref, f3_ref, out_ref, turned_ref):
    g = lax.broadcasted_iota(jnp.int32, (32, 64), 0)
    slot = lax.broadcasted_iota(jnp.int32, (32, 64), 1)
    twice = mm(f2_ref[...], jnp.where(slot // 8 * 4 + slot % 4 == g, 1.0, 0.0).astype(F32))
    flat = image_ref[...].T
    turned_ref[...] = jnp.concatenate([flat[:64], flat[64:]], axis=1)
    bt_high, bt_low = halves(flat)
    z = mm16(jnp.concatenate([bt_high, bt_low], axis=0), high_ref[...])
    z = z[:128] + z[128:] + mm16(bt_high, low_ref[...])
    z = jnp.concatenate(
        [z[:64, t * 128 : t * 128 + 64] + z[64:, t * 128 + 64 : t * 128 + 128] for t in range(8)], axis=1
    ).T
    pieces = [
        jnp.concatenate([z[t * 64 + n * 8 : t * 64 + n * 8 + 8] for t in range(8)], axis=0) for n in range(8)
    ]
    y = mm(twice, jnp.concatenate(pieces, axis=1), 0, 0)
    upper = lax.broadcasted_iota(jnp.int32, (8, 128), 0) < 4
    for f in range(0, 32, 2):
        scale = [jnp.where(upper, f3_ref[c, f], f3_ref[c, f + 1]) for c in range(4)]
        for i in range(8):
            piece = scale[0] * y[i * 8 : i * 8 + 8, :128]
            for c in range(1, 4):
                piece = piece + scale[c] * y[i * 8 : i * 8 + 8, c * 128 : c * 128 + 128]
            out_ref[(i * 32 + f) * 4 : (i * 32 + f) * 4 + 8, :] = piece


def core_body(r_ref, linv_ref, out_ref, kept):
    for i in range(8):
        total = r_ref[i * 128 : i * 128 + 8, :]
        for t in range(1, 16):
            total = total + r_ref[i * 128 + t * 8 : i * 128 + t * 8 + 8, :]
        kept[i * 8 : i * 8 + 8, :] = total + pltpu.roll(total, 4, 0)
    parts = []
    for g in range(4):
        tile = kept[pl.ds(g, 8, stride=8), :]
        parts += [tile[:, :64], tile[:, 64:]]
    out_ref[...] = mm(jnp.concatenate(parts, axis=0), linv_ref[...], 1, 1)


def turn(block, t):
    return lax.ppermute(block, ROW, [(i, (i + t) % 8) for i in range(8)])


def trade(block, axis):
    return lax.all_to_all(block, axis, split_axis=0, concat_axis=0, tiled=True)


def shards(tensor, factor_two, factor_three, factor_four, factor_init):
    x = tensor.reshape(8192, 128)
    me = lax.axis_index(ROW).astype(jnp.int32).reshape(1)
    high, low = call(
        split_body, [((1024, 1024), BF16)] * 2, (HBM, SMEM),
        scratch=(pltpu.VMEM((8192, 128), F32), pltpu.SemaphoreType.DMA((8,))), mib=48, flops=10**8,
    )(x, me)
    *blocks, block = call(
        pack_body, [((512, 128), F32)] * 8 + [((8, 40, 128), F32)], (VMEM,) * 5 + (SMEM,),
        scratch=(pltpu.VMEM((1024, 512), BF16),) * 2, mib=16, flops=3 * 10**9,
    )(high, low, factor_four.T, factor_init.T, factor_two, me)
    block = trade(block, ROW)
    block, f2 = call(
        second_body, [((160, 128), F32), ((64, 32), F32)], (VMEM, VMEM, SMEM), flops=10**7
    )(block, factor_three, me)
    blocks = [blocks[0]] + [turn(blocks[t], t) for t in range(1, 8)]
    block = trade(block.reshape(32, 1, 640), COL)
    (block,) = call(third_body, [((128, 128), F32)], (VMEM,), flops=10**7)(block.reshape(160, 128))
    block = trade(block.reshape(32, 4, 128), COL)
    image, high, low = call(
        image_body, [((512, 128), F32), ((512, 1024), BF16), ((512, 1024), BF16)], (VMEM,) * 10, mib=12, flops=10**9
    )(block.reshape(128, 128), f2, *blocks)
    image = trade(image.reshape(32, 16, 128), PLANE)
    (image,) = call(sum_body, [((8, 16, 128), F32)], (VMEM,), flops=10**6)(image)
    image = trade(image, "z")
    (image,) = call(sum_body, [((32, 16, 128), F32)], (VMEM,), flops=10**6)(image)
    image = trade(image, PLANE)
    block, turned = call(
        core_two_body, [((1024, 128), F32), ((64, 1024), F32)], (VMEM,) * 4 + (SMEM,), mib=12, flops=10**9
    )(image.reshape(512, 128), high, low, f2, factor_three)
    square = mm(turned, turned, 1, 1)
    lower = jnp.linalg.cholesky(square)
    linv = jax.scipy.linalg.solve_triangular(lower, jnp.eye(64, dtype=F32), lower=True)
    basis = mm(linv, turned)
    block = trade(block.reshape(256, 4, 128), ROW + COL)
    (core,) = call(core_body, [((64, 64), F32)], (VMEM, VMEM), scratch=(pltpu.VMEM((64, 128), F32),), flops=10**7)(
        block.reshape(1024, 128), linv
    )
    return basis.T, core.reshape(4, 1, 16, 64).transpose(3, 0, 1, 2)


def solution(mesh):
    split = Mesh(mesh.devices.reshape(4, 2, 4, 8), ("x", "k", "y", "z"))
    in_specs = (P(None, ROW, COL), P(ROW, None), P(COL, None), P(), P())
    out_specs = (P(), P(None, ROW, COL, None))
    return jax.shard_map(shards, mesh=split, in_specs=in_specs, out_specs=out_specs, check_vma=False)
```
